32 devices in a mesh: gx: 4 (over z), gy: 8 (over y, x, core).
Axes of the slice: x: 2, y: 2, z: 4, core: 2. Of those that a mesh axis runs over, the one named last changes fastest.
Arguments:
- substrates: float32 [8, 256, 128, 128], P(None, 'gx', 'gy'), may hold values from 0 to 2
- uptake: float32 [256, 128, 128], P('gx', 'gy'), may hold values from 0.5 to 2
- diffusion: float32 [8], replicated, may hold values from 0.1 to 0.15
- decay_rate: float32 [8], replicated, may hold values from 0.01 to 0.1
Outputs:
- advanced: float32 [8, 256, 128, 128], P(None, 'gx', 'gy')
The draws below stay inside these ranges and needn't reach their ends.
All inputs are finite; a program needn't handle non-finite values.
Results may differ from the reference program's by a relative error of at most 0.00002.
Values sent between devices are 32-bit elements; how exact they have to be, the bound alone decides.
A program may use at most 128 MiB of HBM per device.

```python
import math
import jax
import jax.numpy as jnp

S = 8
CX = 64
CY = 16
CZ = 128
SUBSTEPS = 4
NX = 256
NY = 128


def draw_substrates(key, part):
    first_key, second_key, third_key = jax.random.split(jax.random.fold_in(key, 17), 3)
    grid_shape = (S, NX, NY, CZ)
    x_local = jnp.arange(NX) % CX
    y_local = jnp.arange(NY) % CY
    x_band = (x_local < 4) | (x_local >= CX - 4)
    y_band = (y_local < 4) | (y_local >= CY - 4)
    in_band = (x_band[:, None] | y_band[None, :])[None, :, :, None]
    coin_flips = jax.random.randint(first_key, grid_shape, 0, 2).astype(jnp.float32)
    jitter_values = jax.random.uniform(second_key, grid_shape, jnp.float32)
    inside_draw = jax.random.uniform(third_key, grid_shape, jnp.float32)
    edge_values = 1.6 * coin_flips + 0.4 * jitter_values
    inside_values = 0.4 + 0.4 * inside_draw
    return jnp.where(in_band, edge_values, inside_values).astype(jnp.float32)


def block_scale(own_key, extent, cuts, least, largest):
    factor_of, own = 1.0, jax.random.fold_in(own_key, 6)
    for dim, blocks in cuts:
        steps = jnp.exp(jax.random.uniform(jax.random.fold_in(own, dim), (blocks,), jnp.float32, least / len(cuts), largest / len(cuts)))
        factor_of = factor_of * jnp.repeat(steps, extent[dim] // blocks).reshape([-1 if axis == dim else 1 for axis in range(len(extent))])
    return factor_of


def setup_inputs(seed: int = 0) -> dict:
    splits = jax.random.split(jax.random.key(seed), 5)
    return {
        "substrates": draw_substrates(jax.random.fold_in(splits[4], 71), 0),
        "uptake": jnp.clip(jnp.exp(math.log(2.0) - 1.3862944 * jax.random.uniform(splits[1], (NX, NY, CZ), jnp.float32) ** block_scale(splits[1], (NX, NY, CZ), ((0, 4), (1, 8)), -0.2, 0.2)), 0.5, 2.0),
        "diffusion": jnp.clip(jnp.exp(jax.random.uniform(splits[2], (S,), jnp.float32, math.log(0.1), math.log(0.15))), 0.1, 0.15),
        "decay_rate": jnp.clip(jnp.exp(jax.random.uniform(splits[3], (S,), jnp.float32, math.log(0.01), math.log(0.1))), 0.01, 0.1),
    }


def advance(concentration, uptake, diffuse, decays):
    laplace = jnp.roll(concentration, -1, 1) + jnp.roll(concentration, 1, 1)
    laplace = laplace + jnp.roll(concentration, -1, 2) + jnp.roll(concentration, 1, 2)
    laplace = laplace + jnp.roll(concentration, -1, 3) + jnp.roll(concentration, 1, 3)
    laplace = laplace - 6.0 * concentration
    return concentration + diffuse * laplace - decays * uptake[None] * concentration


def reference(substrates, uptake, diffusion, decay_rate):
    diffuse = diffusion[:, None, None, None]
    decays = decay_rate[:, None, None, None]
    concentration = substrates
    for substep in range(SUBSTEPS):
        concentration = advance(concentration, uptake, diffuse, decays)
    return concentration
```

```python
import functools

import jax
import jax.numpy as jnp
from jax import lax
from jax.experimental import pallas as pl
from jax.experimental.pallas import tpu as pltpu
from jax.sharding import PartitionSpec as P

SUBSTEPS = 4
PITCH_PAD = 16
Y0 = 8
EARLY = 2
MESH = pl.DeviceIdType.MESH


def kernel(
    n_x, n_y, sub_ref, up_ref, dif_hbm, dec_hbm, out_ref,
    field, uptake, faces, halos, load_sem, up_sem, send_sem, recv_sem,
    dif_ref, dec_ref, scalar_sem, ready,
):
    count, cx, cy, cz = sub_ref.shape
    pitch = cy + PITCH_PAD
    rows = field.reshape(SUBSTEPS, count, (cx + 2) * pitch, cz)
    gx, gy = lax.axis_index("gx"), lax.axis_index("gy")
    low_x, high_x = lax.rem(gx + n_x - 1, n_x), lax.rem(gx + 1, n_x)
    low_y, high_y = lax.rem(gy + n_y - 1, n_y), lax.rem(gy + 1, n_y)
    inner = pl.ds(Y0, cy)
    along_x = (low_x, high_x)

    def load(s):
        return pltpu.make_async_copy(
            sub_ref.at[s], field.at[0, s, pl.ds(1, cx), inner, :], load_sem.at[s]
        )

    def remote(t, s, k, src, dst, target):
        return pltpu.make_async_remote_copy(
            src_ref=src, dst_ref=dst, send_sem=send_sem.at[t, s, k],
            recv_sem=recv_sem.at[t, s, k], device_id=target, device_id_type=MESH,
        )

    def y_sends(t, s):
        return [
            remote(t, s, 0, faces.at[t, s, 0], halos.at[t, s, 0], (gx, low_y)),
            remote(t, s, 1, faces.at[t, s, 1], halos.at[t, s, 1], (gx, high_y)),
        ]

    def x_sends(t, s):
        here = field.at[t, s]
        return [
            remote(t, s, 2, here.at[1, inner, :], here.at[cx + 1, inner, :], (low_x, gy)),
            remote(t, s, 3, here.at[cx, inner, :], here.at[0, inner, :], (high_x, gy)),
        ]

    def sends(t, s):
        return y_sends(t, s) + x_sends(t, s)

    def make_faces(t, s):
        for i in range(cx // 8):
            top = (1 + 8 * i) * pitch + Y0
            faces[t, s, 0, pl.ds(8 * i, 8), :] = rows[t, s, pl.ds(top, 8, stride=pitch), :]
            faces[t, s, 1, pl.ds(8 * i, 8), :] = rows[
                t, s, pl.ds(top + cy - 1, 8, stride=pitch), :
            ]

    def unit(t, s):
        for copy in sends(t, s):
            copy.wait_recv()
        for i in range(cx // 8):
            top = (1 + 8 * i) * pitch + Y0
            rows[t, s, pl.ds(top + cy, 8, stride=pitch), :] = halos[t, s, 0, pl.ds(8 * i, 8), :]
            rows[t, s, pl.ds(top - 1, 8, stride=pitch), :] = halos[t, s, 1, pl.ds(8 * i, 8), :]
        diffuse = dif_ref[s]
        keep = 1.0 - 6.0 * diffuse
        decay = dec_ref[s]
        for y in range(0, cy, 8):
            below = field[t, s, 0, pl.ds(Y0 + y, 8), :]
            center = field[t, s, 1, pl.ds(Y0 + y, 8), :]
            for x in range(cx):
                above = field[t, s, x + 2, pl.ds(Y0 + y, 8), :]
                total = below + above
                total = total + (
                    field[t, s, x + 1, pl.ds(Y0 + y - 1, 8), :]
                    + field[t, s, x + 1, pl.ds(Y0 + y + 1, 8), :]
                )
                total = total + (pltpu.roll(center, 1, 1) + pltpu.roll(center, cz - 1, 1))
                factor = keep - decay * uptake[x, pl.ds(y, 8), :]
                value = diffuse * total + factor * center
                if t + 1 < SUBSTEPS:
                    field[t + 1, s, x + 1, pl.ds(Y0 + y, 8), :] = value
                else:
                    out_ref[s, x, pl.ds(y, 8), :] = value
                below, center = center, above

    def run(first, last, body):
        def wrapped(s, carry):
            body(s)
            return carry

        lax.fori_loop(first, last, wrapped, 0)

    barrier = pltpu.get_barrier_semaphore()
    for target in ((gx, low_y), (gx, high_y)):
        pl.semaphore_signal(barrier, inc=1, device_id=target, device_id_type=MESH)
    for other in along_x:

        @pl.when(other > gx)
        def _():
            pl.semaphore_signal(barrier, inc=1, device_id=(other, gy), device_id_type=MESH)

    run(0, count, lambda s: load(s).start())
    up_copy = pltpu.make_async_copy(up_ref, uptake, up_sem)
    up_copy.start()
    scalar_copies = [
        pltpu.make_async_copy(dif_hbm, dif_ref, scalar_sem.at[0]),
        pltpu.make_async_copy(dec_hbm, dec_ref, scalar_sem.at[1]),
    ]
    for copy in scalar_copies:
        copy.start()

    def fetch(s):
        load(s).wait()
        make_faces(0, s)

    def launch(s):
        for copy in y_sends(0, s):
            copy.start()
        for other, copy in zip(along_x, x_sends(0, s)):

            @pl.when(other < gx)
            def _():
                copy.start()

    run(0, EARLY, fetch)
    n_lower = sum((other < gx).astype(jnp.int32) for other in along_x)
    pl.semaphore_wait(barrier, 2 + n_lower)
    for k, other in enumerate(along_x):

        @pl.when(other < gx)
        def _():
            pl.semaphore_signal(
                ready.at[1 - k], inc=1, device_id=(other, gy), device_id_type=MESH
            )

    run(0, EARLY, launch)

    def fetch_and_launch(s):
        fetch(s)
        launch(s)

    run(EARLY, count, fetch_and_launch)
    for k, other in enumerate(along_x):

        @pl.when(other > gx)
        def _():
            pl.semaphore_wait(ready.at[k], 1)
            run(0, count, lambda s: x_sends(0, s)[k].start())

    up_copy.wait()
    for copy in scalar_copies:
        copy.wait()
    for t in range(SUBSTEPS):

        def advance(s):
            unit(t, s)
            if t + 1 < SUBSTEPS:
                make_faces(t + 1, s)
                for copy in sends(t + 1, s):
                    copy.start()
            if t > 0:
                for copy in sends(t - 1, s):
                    copy.wait_send()

        run(0, count, advance)

    def finish(s):
        for copy in sends(SUBSTEPS - 1, s):
            copy.wait_send()

    run(0, count, finish)


def solution(mesh):
    n_x, n_y = mesh.shape["gx"], mesh.shape["gy"]

    def local(substrates, uptake, diffusion, decay_rate):
        count, cx, cy, cz = substrates.shape
        hbm_spec = pl.BlockSpec(memory_space=pltpu.HBM)
        return pl.pallas_call(
            functools.partial(kernel, n_x, n_y),
            out_shape=jax.ShapeDtypeStruct(substrates.shape, substrates.dtype),
            in_specs=[hbm_spec] * 4,
            out_specs=pl.BlockSpec(memory_space=pltpu.VMEM),
            scratch_shapes=[
                pltpu.VMEM((SUBSTEPS, count, cx + 2, cy + PITCH_PAD, cz), jnp.float32),
                pltpu.VMEM((cx, cy, cz), jnp.float32),
                pltpu.VMEM((SUBSTEPS, count, 2, cx, cz), jnp.float32),
                pltpu.VMEM((SUBSTEPS, count, 2, cx, cz), jnp.float32),
                pltpu.SemaphoreType.DMA((count,)),
                pltpu.SemaphoreType.DMA,
                pltpu.SemaphoreType.DMA((SUBSTEPS, count, 4)),
                pltpu.SemaphoreType.DMA((SUBSTEPS, count, 4)),
                pltpu.SMEM((count,), jnp.float32),
                pltpu.SMEM((count,), jnp.float32),
                pltpu.SemaphoreType.DMA((2,)),
                pltpu.SemaphoreType.REGULAR((2,)),
            ],
            compiler_params=pltpu.CompilerParams(
                collective_id=0, has_side_effects=True, vmem_limit_bytes=44 * 1024 * 1024
            ),
        )(*[pltpu.with_memory_space_constraint(v, pltpu.HBM) for v in (substrates, uptake, diffusion, decay_rate)])

    placed = (P(None, "gx", "gy", None), P("gx", "gy", None), P(), P())
    return jax.shard_map(
        local, mesh=mesh, in_specs=placed, out_specs=P(None, "gx", "gy", None), check_vma=False
    )
```

```python
import functools

import jax
import jax.numpy as jnp
from jax import lax
from jax.experimental import pallas as pl
from jax.experimental.pallas import tpu as pltpu
from jax.sharding import PartitionSpec as P

SUBSTEPS = 4
PITCH_PAD = 16
Y0 = 8
EARLY = 2
MESH = pl.DeviceIdType.MESH


def kernel(
    n_x, n_y, sub_ref, up_ref, dif_hbm, dec_hbm, out_ref,
    field, uptake, faces, halos, front_sem, bulk_sem, up_sem, send_sem, recv_sem,
    dif_ref, dec_ref, scalar_sem, ready,
):
    count, cx, cy, cz = sub_ref.shape
    pitch = cy + PITCH_PAD
    rows = field.reshape(SUBSTEPS, count, (cx + 2) * pitch, cz)
    gx, gy = lax.axis_index("gx"), lax.axis_index("gy")
    low_x, high_x = lax.rem(gx + n_x - 1, n_x), lax.rem(gx + 1, n_x)
    low_y, high_y = lax.rem(gy + n_y - 1, n_y), lax.rem(gy + 1, n_y)
    inner = pl.ds(Y0, cy)
    along_x = (low_x, high_x)

    shell = 2 * (cx + cy)
    flat = field.reshape(SUBSTEPS * count * (cx + 2) * pitch, cz)

    def front(s, group):
        pairs = (
            (sub_ref.at[s, :, 0, :], faces.at[0, s, 0]),
            (sub_ref.at[s, :, cy - 1, :], faces.at[0, s, 1]),
            (sub_ref.at[s, 0], field.at[0, s, 1, inner, :]),
            (sub_ref.at[s, cx - 1], field.at[0, s, cx, inner, :]),
        )
        return [pltpu.make_async_copy(src, dst, front_sem.at[group]) for src, dst in pairs]

    def bulk(s):
        return pltpu.make_async_copy(
            sub_ref.at[s, pl.ds(1, cx - 2)], field.at[0, s, pl.ds(2, cx - 2), inner, :], bulk_sem
        )

    def await_rows(n, sem):
        span = flat.at[pl.ds(0, n), :]
        pltpu.make_async_copy(span, span, sem).wait()

    def remote(t, s, src, dst, target):
        return pltpu.make_async_remote_copy(
            src_ref=src, dst_ref=dst, send_sem=send_sem.at[t],
            recv_sem=recv_sem.at[t % 2, s], device_id=target, device_id_type=MESH,
        )

    def y_sends(t, s):
        return [
            remote(t, s, faces.at[t, s, 0], halos.at[t, s, 0], (gx, low_y)),
            remote(t, s, faces.at[t, s, 1], halos.at[t, s, 1], (gx, high_y)),
        ]

    def x_send(t, s, k):
        here = field.at[t, s]
        if k == 0:
            return remote(t, s, here.at[1, inner, :], here.at[cx + 1, inner, :], (low_x, gy))
        return remote(t, s, here.at[cx, inner, :], here.at[0, inner, :], (high_x, gy))

    def sends(t, s):
        return y_sends(t, s) + [x_send(t, s, 0), x_send(t, s, 1)]

    def make_faces(t, s):
        for i in range(cx // 8):
            top = (1 + 8 * i) * pitch + Y0
            faces[t, s, 0, pl.ds(8 * i, 8), :] = rows[t, s, pl.ds(top, 8, stride=pitch), :]
            faces[t, s, 1, pl.ds(8 * i, 8), :] = rows[
                t, s, pl.ds(top + cy - 1, 8, stride=pitch), :
            ]

    def unit(t, s):
        await_rows(shell, recv_sem.at[t % 2, s])
        for i in range(cx // 8):
            top = (1 + 8 * i) * pitch + Y0
            rows[t, s, pl.ds(top + cy, 8, stride=pitch), :] = halos[t, s, 0, pl.ds(8 * i, 8), :]
            rows[t, s, pl.ds(top - 1, 8, stride=pitch), :] = halos[t, s, 1, pl.ds(8 * i, 8), :]
        diffuse = dif_ref[s]
        keep = 1.0 - 6.0 * diffuse
        decay = dec_ref[s]
        for y in range(0, cy, 8):
            below = field[t, s, 0, pl.ds(Y0 + y, 8), :]
            center = field[t, s, 1, pl.ds(Y0 + y, 8), :]
            for x in range(cx):
                above = field[t, s, x + 2, pl.ds(Y0 + y, 8), :]
                total = below + above
                total = total + (
                    field[t, s, x + 1, pl.ds(Y0 + y - 1, 8), :]
                    + field[t, s, x + 1, pl.ds(Y0 + y + 1, 8), :]
                )
                total = total + (pltpu.roll(center, 1, 1) + pltpu.roll(center, cz - 1, 1))
                factor = keep - decay * uptake[x, pl.ds(y, 8), :]
                value = diffuse * total + factor * center
                if t + 1 < SUBSTEPS:
                    field[t + 1, s, x + 1, pl.ds(Y0 + y, 8), :] = value
                else:
                    out_ref[s, x, pl.ds(y, 8), :] = value
                below, center = center, above

    def run(first, last, body):
        def wrapped(s, carry):
            body(s)
            return carry

        lax.fori_loop(first, last, wrapped, 0)

    barrier = pltpu.get_barrier_semaphore()
    for target in ((gx, low_y), (gx, high_y)):
        pl.semaphore_signal(barrier, inc=1, device_id=target, device_id_type=MESH)
    for other in along_x:

        @pl.when(other > gx)
        def _():
            pl.semaphore_signal(barrier, inc=1, device_id=(other, gy), device_id_type=MESH)

    for first, last, group in ((0, EARLY, 0), (EARLY, count, 1)):

        def begin(s):
            for copy in front(s, group):
                copy.start()

        run(first, last, begin)
    scalar_copies = [
        pltpu.make_async_copy(dif_hbm, dif_ref, scalar_sem.at[0]),
        pltpu.make_async_copy(dec_hbm, dec_ref, scalar_sem.at[1]),
    ]
    for copy in scalar_copies:
        copy.start()
    run(0, count, lambda s: bulk(s).start())
    up_copy = pltpu.make_async_copy(up_ref, uptake, up_sem)
    up_copy.start()

    def launch(s):
        for copy in y_sends(0, s):
            copy.start()
        for k, other in enumerate(along_x):

            @pl.when(other < gx)
            def _():
                x_send(0, s, k).start()

    n_lower = sum((other < gx).astype(jnp.int32) for other in along_x)
    pl.semaphore_wait(barrier, 2 + n_lower)
    for k, other in enumerate(along_x):

        @pl.when(other < gx)
        def _():
            pl.semaphore_signal(
                ready.at[1 - k], inc=1, device_id=(other, gy), device_id_type=MESH
            )

    for first, last, group in ((0, EARLY, 0), (EARLY, count, 1)):
        await_rows((last - first) * shell, front_sem.at[group])
        run(first, last, launch)
    for k, other in enumerate(along_x):

        @pl.when(other > gx)
        def _():
            pl.semaphore_wait(ready.at[k], 1)
            run(0, count, lambda s: x_send(0, s, k).start())

    await_rows(count * (cx - 2) * cy, bulk_sem)
    up_copy.wait()
    for copy in scalar_copies:
        copy.wait()
    for t in range(SUBSTEPS):

        def advance(s):
            unit(t, s)
            if t + 1 < SUBSTEPS:
                make_faces(t + 1, s)
                for copy in sends(t + 1, s):
                    copy.start()

        run(0, count, advance)

    for t in range(SUBSTEPS):
        await_rows(count * shell, send_sem.at[t])


def solution(mesh):
    n_x, n_y = mesh.shape["gx"], mesh.shape["gy"]

    def local(substrates, uptake, diffusion, decay_rate):
        count, cx, cy, cz = substrates.shape
        hbm_spec = pl.BlockSpec(memory_space=pltpu.HBM)
        return pl.pallas_call(
            functools.partial(kernel, n_x, n_y),
            out_shape=jax.ShapeDtypeStruct(substrates.shape, substrates.dtype),
            in_specs=[hbm_spec] * 4,
            out_specs=pl.BlockSpec(memory_space=pltpu.VMEM),
            scratch_shapes=[
                pltpu.VMEM((SUBSTEPS, count, cx + 2, cy + PITCH_PAD, cz), jnp.float32),
                pltpu.VMEM((cx, cy, cz), jnp.float32),
                pltpu.VMEM((SUBSTEPS, count, 2, cx, cz), jnp.float32),
                pltpu.VMEM((SUBSTEPS, count, 2, cx, cz), jnp.float32),
                pltpu.SemaphoreType.DMA((2,)),
                pltpu.SemaphoreType.DMA,
                pltpu.SemaphoreType.DMA,
                pltpu.SemaphoreType.DMA((SUBSTEPS,)),
                pltpu.SemaphoreType.DMA((2, count)),
                pltpu.SMEM((count,), jnp.float32),
                pltpu.SMEM((count,), jnp.float32),
                pltpu.SemaphoreType.DMA((2,)),
                pltpu.SemaphoreType.REGULAR((2,)),
            ],
            compiler_params=pltpu.CompilerParams(
                collective_id=0, has_side_effects=True, vmem_limit_bytes=44 * 1024 * 1024
            ),
        )(*[pltpu.with_memory_space_constraint(v, pltpu.HBM) for v in (substrates, uptake, diffusion, decay_rate)])

    placed = (P(None, "gx", "gy", None), P("gx", "gy", None), P(), P())
    return jax.shard_map(
        local, mesh=mesh, in_specs=placed, out_specs=P(None, "gx", "gy", None), check_vma=False
    )
```

```python
import functools

import jax
import jax.numpy as jnp
from jax import lax
from jax.experimental import pallas as pl
from jax.experimental.pallas import tpu as pltpu
from jax.sharding import PartitionSpec as P

SUBSTEPS = 4
PITCH_PAD = 16
Y0 = 8
EARLY = 2
MESH = pl.DeviceIdType.MESH


def kernel(
    n_x, n_y, sub_ref, up_ref, dif_hbm, dec_hbm, out_ref,
    field, uptake, faces, halos, front_sem, bulk_sem, up_sem, send_sem, recv_sem,
    dif_ref, dec_ref, scalar_sem, ready,
):
    count, cx, cy, cz = sub_ref.shape
    pitch = cy + PITCH_PAD
    rows = field.reshape(SUBSTEPS, count, (cx + 2) * pitch, cz)
    gx, gy = lax.axis_index("gx"), lax.axis_index("gy")
    low_x, high_x = lax.rem(gx + n_x - 1, n_x), lax.rem(gx + 1, n_x)
    low_y, high_y = lax.rem(gy + n_y - 1, n_y), lax.rem(gy + 1, n_y)
    inner = pl.ds(Y0, cy)
    along_x = (low_x, high_x)

    shell = 2 * (cx + cy)
    flat = field.reshape(SUBSTEPS * count * (cx + 2) * pitch, cz)

    def front(s, group):
        pairs = (
            (sub_ref.at[s, :, 0, :], faces.at[0, s, 0]),
            (sub_ref.at[s, :, cy - 1, :], faces.at[0, s, 1]),
            (sub_ref.at[s, 0], field.at[0, s, 1, inner, :]),
            (sub_ref.at[s, cx - 1], field.at[0, s, cx, inner, :]),
        )
        return [pltpu.make_async_copy(src, dst, front_sem.at[group]) for src, dst in pairs]

    def bulk(s):
        return pltpu.make_async_copy(
            sub_ref.at[s, pl.ds(1, cx - 2)], field.at[0, s, pl.ds(2, cx - 2), inner, :], bulk_sem
        )

    def await_rows(n, sem):
        span = flat.at[pl.ds(0, n), :]
        pltpu.make_async_copy(span, span, sem).wait()

    def remote(t, s, src, dst, target):
        return pltpu.make_async_remote_copy(
            src_ref=src, dst_ref=dst, send_sem=send_sem.at[t],
            recv_sem=recv_sem.at[t % 2, s], device_id=target, device_id_type=MESH,
        )

    def y_sends(t, s):
        return [
            remote(t, s, faces.at[t, s, 0], halos.at[t, s, 0], (gx, low_y)),
            remote(t, s, faces.at[t, s, 1], halos.at[t, s, 1], (gx, high_y)),
        ]

    def x_send(t, s, k):
        here = field.at[t, s]
        if k == 0:
            return remote(t, s, here.at[1, inner, :], here.at[cx + 1, inner, :], (low_x, gy))
        return remote(t, s, here.at[cx, inner, :], here.at[0, inner, :], (high_x, gy))

    def sends(t, s):
        return y_sends(t, s) + [x_send(t, s, 0), x_send(t, s, 1)]

    def make_faces(t, s):
        for i in range(cx // 8):
            top = (1 + 8 * i) * pitch + Y0
            faces[t, s, 0, pl.ds(8 * i, 8), :] = rows[t, s, pl.ds(top, 8, stride=pitch), :]
            faces[t, s, 1, pl.ds(8 * i, 8), :] = rows[
                t, s, pl.ds(top + cy - 1, 8, stride=pitch), :
            ]

    def unit(t, s):
        await_rows(shell, recv_sem.at[t % 2, s])
        for i in range(cx // 8):
            top = (1 + 8 * i) * pitch + Y0
            rows[t, s, pl.ds(top + cy, 8, stride=pitch), :] = halos[t, s, 0, pl.ds(8 * i, 8), :]
            rows[t, s, pl.ds(top - 1, 8, stride=pitch), :] = halos[t, s, 1, pl.ds(8 * i, 8), :]
        diffuse = dif_ref[s]
        keep = 1.0 - 6.0 * diffuse
        decay = dec_ref[s]
        for y in range(0, cy, 8):
            below = field[t, s, 0, pl.ds(Y0 + y, 8), :]
            center = field[t, s, 1, pl.ds(Y0 + y, 8), :]
            for x in range(cx):
                above = field[t, s, x + 2, pl.ds(Y0 + y, 8), :]
                total = below + above
                total = total + (
                    field[t, s, x + 1, pl.ds(Y0 + y - 1, 8), :]
                    + field[t, s, x + 1, pl.ds(Y0 + y + 1, 8), :]
                )
                total = total + (pltpu.roll(center, 1, 1) + pltpu.roll(center, cz - 1, 1))
                factor = keep - decay * uptake[x, pl.ds(y, 8), :]
                value = diffuse * total + factor * center
                if t + 1 < SUBSTEPS:
                    field[t + 1, s, x + 1, pl.ds(Y0 + y, 8), :] = value
                else:
                    out_ref[s, x, pl.ds(y, 8), :] = value
                below, center = center, above

    def run(first, last, body):
        def wrapped(s, carry):
            body(s)
            return carry

        lax.fori_loop(first, last, wrapped, 0)

    barrier = pltpu.get_barrier_semaphore()
    for target in ((gx, low_y), (gx, high_y)):
        pl.semaphore_signal(barrier, inc=1, device_id=target, device_id_type=MESH)
    for other in along_x:

        @pl.when(other > gx)
        def _():
            pl.semaphore_signal(barrier, inc=1, device_id=(other, gy), device_id_type=MESH)

    for first, last, group in ((0, EARLY, 0), (EARLY, count, 1)):

        def begin(s):
            for copy in front(s, group):
                copy.start()

        run(first, last, begin)
    scalar_copies = [
        pltpu.make_async_copy(dif_hbm, dif_ref, scalar_sem.at[0]),
        pltpu.make_async_copy(dec_hbm, dec_ref, scalar_sem.at[1]),
    ]
    for copy in scalar_copies:
        copy.start()
    run(0, count, lambda s: bulk(s).start())
    up_copy = pltpu.make_async_copy(up_ref, uptake, up_sem)
    up_copy.start()

    def launch(s):
        for copy in y_sends(0, s):
            copy.start()
        for k, other in enumerate(along_x):

            @pl.when(other < gx)
            def _():
                x_send(0, s, k).start()

    n_lower = sum((other < gx).astype(jnp.int32) for other in along_x)
    pl.semaphore_wait(barrier, 2 + n_lower)
    for k, other in enumerate(along_x):

        @pl.when(other < gx)
        def _():
            pl.semaphore_signal(
                ready.at[1 - k], inc=1, device_id=(other, gy), device_id_type=MESH
            )

    for first, last, group in ((0, EARLY, 0), (EARLY, count, 1)):
        await_rows((last - first) * shell, front_sem.at[group])
        run(first, last, launch)
    for k, other in ((1, high_x), (0, low_x)):

        @pl.when(other > gx)
        def _():
            pl.semaphore_wait(ready.at[k], 1)
            run(0, count, lambda s: x_send(0, s, k).start())

    await_rows(count * (cx - 2) * cy, bulk_sem)
    up_copy.wait()
    for copy in scalar_copies:
        copy.wait()
    for t in range(SUBSTEPS):

        def advance(s):
            unit(t, s)
            if t + 1 < SUBSTEPS:
                make_faces(t + 1, s)
                for copy in sends(t + 1, s):
                    copy.start()

        run(0, count, advance)

    for t in range(SUBSTEPS):
        await_rows(count * shell, send_sem.at[t])


def solution(mesh):
    n_x, n_y = mesh.shape["gx"], mesh.shape["gy"]

    def local(substrates, uptake, diffusion, decay_rate):
        count, cx, cy, cz = substrates.shape
        hbm_spec = pl.BlockSpec(memory_space=pltpu.HBM)
        return pl.pallas_call(
            functools.partial(kernel, n_x, n_y),
            out_shape=jax.ShapeDtypeStruct(substrates.shape, substrates.dtype),
            in_specs=[hbm_spec] * 4,
            out_specs=pl.BlockSpec(memory_space=pltpu.VMEM),
            scratch_shapes=[
                pltpu.VMEM((SUBSTEPS, count, cx + 2, cy + PITCH_PAD, cz), jnp.float32),
                pltpu.VMEM((cx, cy, cz), jnp.float32),
                pltpu.VMEM((SUBSTEPS, count, 2, cx, cz), jnp.float32),
                pltpu.VMEM((SUBSTEPS, count, 2, cx, cz), jnp.float32),
                pltpu.SemaphoreType.DMA((2,)),
                pltpu.SemaphoreType.DMA,
                pltpu.SemaphoreType.DMA,
                pltpu.SemaphoreType.DMA((SUBSTEPS,)),
                pltpu.SemaphoreType.DMA((2, count)),
                pltpu.SMEM((count,), jnp.float32),
                pltpu.SMEM((count,), jnp.float32),
                pltpu.SemaphoreType.DMA((2,)),
                pltpu.SemaphoreType.REGULAR((2,)),
            ],
            compiler_params=pltpu.CompilerParams(
                collective_id=0, has_side_effects=True, vmem_limit_bytes=44 * 1024 * 1024
            ),
        )(*[pltpu.with_memory_space_constraint(v, pltpu.HBM) for v in (substrates, uptake, diffusion, decay_rate)])

    placed = (P(None, "gx", "gy", None), P("gx", "gy", None), P(), P())
    return jax.shard_map(
        local, mesh=mesh, in_specs=placed, out_specs=P(None, "gx", "gy", None), check_vma=False
    )
```

```python
import functools

import jax
import jax.numpy as jnp
from jax import lax
from jax.experimental import pallas as pl
from jax.experimental.pallas import tpu as pltpu
from jax.sharding import PartitionSpec as P

SUBSTEPS = 4
PITCH_PAD = 16
Y0 = 8
EARLY = 2
MESH = pl.DeviceIdType.MESH


def kernel(
    n_x, n_y, sub_ref, up_ref, dif_hbm, dec_hbm, out_ref,
    field, uptake, faces, halos, front_sem, bulk_sem, send_sem, recv_sem,
    dif_ref, dec_ref, ready,
):
    count, cx, cy, cz = sub_ref.shape
    pitch = cy + PITCH_PAD
    out_rows = out_ref.reshape(count, cx * cy, cz)
    rows = field.reshape(SUBSTEPS, count, (cx + 2) * pitch, cz)
    gx, gy = lax.axis_index("gx"), lax.axis_index("gy")
    low_x, high_x = lax.rem(gx + n_x - 1, n_x), lax.rem(gx + 1, n_x)
    low_y, high_y = lax.rem(gy + n_y - 1, n_y), lax.rem(gy + 1, n_y)
    inner = pl.ds(Y0, cy)
    along_x = (low_x, high_x)

    shell = 2 * (cx + cy)
    flat = field.reshape(SUBSTEPS * count * (cx + 2) * pitch, cz)

    def front(s, group):
        pairs = (
            (sub_ref.at[s, :, 0, :], faces.at[0, s, 0]),
            (sub_ref.at[s, :, cy - 1, :], faces.at[0, s, 1]),
            (sub_ref.at[s, 0], field.at[0, s, 1, inner, :]),
            (sub_ref.at[s, cx - 1], field.at[0, s, cx, inner, :]),
        )
        return [pltpu.make_async_copy(src, dst, front_sem.at[group]) for src, dst in pairs]

    def bulk(s):
        return pltpu.make_async_copy(
            sub_ref.at[s, pl.ds(1, cx - 2)], field.at[0, s, pl.ds(2, cx - 2), inner, :], bulk_sem
        )

    def await_rows(n, sem):
        span = flat.at[pl.ds(0, n), :]
        pltpu.make_async_copy(span, span, sem).wait()

    def remote(t, s, src, dst, target):
        return pltpu.make_async_remote_copy(
            src_ref=src, dst_ref=dst, send_sem=send_sem,
            recv_sem=recv_sem.at[t % 2, s], device_id=target, device_id_type=MESH,
        )

    def y_sends(t, s):
        return [
            remote(t, s, faces.at[t, s, 0], halos.at[t, s, 0], (gx, low_y)),
            remote(t, s, faces.at[t, s, 1], halos.at[t, s, 1], (gx, high_y)),
        ]

    def x_send(t, s, k):
        here = field.at[t, s]
        if k == 0:
            return remote(t, s, here.at[1, inner, :], here.at[cx + 1, inner, :], (low_x, gy))
        return remote(t, s, here.at[cx, inner, :], here.at[0, inner, :], (high_x, gy))

    def make_faces(t, s):
        for i in range(cx // 8):
            top = (1 + 8 * i) * pitch + Y0
            faces[t, s, 0, pl.ds(8 * i, 8), :] = rows[t, s, pl.ds(top, 8, stride=pitch), :]
            faces[t, s, 1, pl.ds(8 * i, 8), :] = rows[
                t, s, pl.ds(top + cy - 1, 8, stride=pitch), :
            ]

    def step(t, s, ghosts, first=0, last=None):
        last = cx if last is None else last
        diffuse = dif_ref[s]
        keep = 1.0 - 6.0 * diffuse
        decay = dec_ref[s]
        zero = jnp.zeros((8, cz), jnp.float32)
        sublane = lax.broadcasted_iota(jnp.int32, (8, cz), 0)
        for y in range(0, cy, 8):
            below = field[t, s, first, pl.ds(Y0 + y, 8), :] if ghosts else zero
            center = field[t, s, first + 1, pl.ds(Y0 + y, 8), :]
            for x in range(first, last):
                if ghosts or x + 1 < cx:
                    above = field[t, s, x + 2, pl.ds(Y0 + y, 8), :]
                else:
                    above = zero
                total = below + above
                left = field[t, s, x + 1, pl.ds(Y0 + y - 1, 8), :]
                right = field[t, s, x + 1, pl.ds(Y0 + y + 1, 8), :]
                if not ghosts and y == 0:
                    left = jnp.where(sublane == 0, 0.0, left)
                if not ghosts and y + 8 == cy:
                    right = jnp.where(sublane == 7, 0.0, right)
                total = total + (left + right)
                total = total + (pltpu.roll(center, 1, 1) + pltpu.roll(center, cz - 1, 1))
                factor = keep - decay * uptake[x, pl.ds(y, 8), :]
                value = diffuse * total + factor * center
                if t + 1 < SUBSTEPS:
                    field[t + 1, s, x + 1, pl.ds(Y0 + y, 8), :] = value
                else:
                    out_ref[s, x, pl.ds(y, 8), :] = value
                below, center = center, above

    def unit(t, s):
        await_rows(shell, recv_sem.at[t % 2, s])
        for i in range(cx // 8):
            top = (1 + 8 * i) * pitch + Y0
            rows[t, s, pl.ds(top + cy, 8, stride=pitch), :] = halos[t, s, 0, pl.ds(8 * i, 8), :]
            rows[t, s, pl.ds(top - 1, 8, stride=pitch), :] = halos[t, s, 1, pl.ds(8 * i, 8), :]
        step(t, s, True, 0, 1)
        step(t, s, True, cx - 1, cx)
        for k in range(2):
            x_send(t + 1, s, k).start()
        step(t, s, True, 1, cx - 1)
        make_faces(t + 1, s)
        for copy in y_sends(t + 1, s):
            copy.start()

    def last_unit(t, s):
        step(t, s, False)
        await_rows(shell, recv_sem.at[t % 2, s])
        diffuse = dif_ref[s]
        for x, ghost in ((0, 0), (cx - 1, cx + 1)):
            out_ref[s, x] += diffuse * field[t, s, ghost, inner, :]
        for i in range(cx // 8):
            for k, y in ((0, cy - 1), (1, 0)):
                edge = pl.ds(8 * i * cy + y, 8, stride=cy)
                out_rows[s, edge, :] += diffuse * halos[t, s, k, pl.ds(8 * i, 8), :]

    def run(first, last, body):
        def wrapped(s, carry):
            body(s)
            return carry

        lax.fori_loop(first, last, wrapped, 0)

    barrier = pltpu.get_barrier_semaphore()
    for target in ((gx, low_y), (gx, high_y)):
        pl.semaphore_signal(barrier, inc=1, device_id=target, device_id_type=MESH)
    for other in along_x:

        @pl.when(other > gx)
        def _():
            pl.semaphore_signal(barrier, inc=1, device_id=(other, gy), device_id_type=MESH)

    for first, last, group in ((0, EARLY, 0), (EARLY, count, 1)):

        def begin(s):
            for copy in front(s, group):
                copy.start()

        run(first, last, begin)
    run(0, count, lambda s: bulk(s).start())
    pltpu.make_async_copy(up_ref, uptake, bulk_sem).start()

    def launch(s):
        for copy in y_sends(0, s):
            copy.start()
        for k, other in enumerate(along_x):

            @pl.when(other < gx)
            def _():
                x_send(0, s, k).start()

    n_lower = sum((other < gx).astype(jnp.int32) for other in along_x)
    pl.semaphore_wait(barrier, 2 + n_lower)
    for k, other in enumerate(along_x):

        @pl.when(other < gx)
        def _():
            pl.semaphore_signal(
                ready.at[1 - k], inc=1, device_id=(other, gy), device_id_type=MESH
            )

    for first, last, group in ((0, EARLY, 0), (EARLY, count, 1)):
        await_rows((last - first) * shell, front_sem.at[group])
        run(first, last, launch)
    scalar_copies = [
        pltpu.make_async_copy(dif_hbm, dif_ref, front_sem.at[0]),
        pltpu.make_async_copy(dec_hbm, dec_ref, front_sem.at[1]),
    ]
    for copy in scalar_copies:
        copy.start()
    for k, other in ((1, high_x), (0, low_x)):

        @pl.when(other > gx)
        def _():
            pl.semaphore_wait(ready.at[k], 1)
            run(0, count, lambda s: x_send(0, s, k).start())

    await_rows(count * (cx - 2) * cy + cx * cy, bulk_sem)
    for copy in scalar_copies:
        copy.wait()
    for t in range(SUBSTEPS - 1):
        run(0, count, lambda s: unit(t, s))
    run(0, count, lambda s: last_unit(SUBSTEPS - 1, s))
    await_rows(SUBSTEPS * count * shell, send_sem)


def solution(mesh):
    n_x, n_y = mesh.shape["gx"], mesh.shape["gy"]

    def local(substrates, uptake, diffusion, decay_rate):
        count, cx, cy, cz = substrates.shape
        hbm_spec = pl.BlockSpec(memory_space=pltpu.HBM)
        return pl.pallas_call(
            functools.partial(kernel, n_x, n_y),
            out_shape=jax.ShapeDtypeStruct(substrates.shape, substrates.dtype),
            in_specs=[hbm_spec] * 4,
            out_specs=pl.BlockSpec(memory_space=pltpu.VMEM),
            scratch_shapes=[
                pltpu.VMEM((SUBSTEPS, count, cx + 2, cy + PITCH_PAD, cz), jnp.float32),
                pltpu.VMEM((cx, cy, cz), jnp.float32),
                pltpu.VMEM((SUBSTEPS, count, 2, cx, cz), jnp.float32),
                pltpu.VMEM((SUBSTEPS, count, 2, cx, cz), jnp.float32),
                pltpu.SemaphoreType.DMA((2,)),
                pltpu.SemaphoreType.DMA,
                pltpu.SemaphoreType.DMA,
                pltpu.SemaphoreType.DMA((2, count)),
                pltpu.SMEM((count,), jnp.float32),
                pltpu.SMEM((count,), jnp.float32),
                pltpu.SemaphoreType.REGULAR((2,)),
            ],
            compiler_params=pltpu.CompilerParams(
                collective_id=0, has_side_effects=True, vmem_limit_bytes=44 * 1024 * 1024
            ),
        )(*[pltpu.with_memory_space_constraint(v, pltpu.HBM) for v in (substrates, uptake, diffusion, decay_rate)])

    placed = (P(None, "gx", "gy", None), P("gx", "gy", None), P(), P())
    return jax.shard_map(
        local, mesh=mesh, in_specs=placed, out_specs=P(None, "gx", "gy", None), check_vma=False
    )
```

```python
import functools

import jax
import jax.numpy as jnp
from jax import lax
from jax.experimental import pallas as pl
from jax.experimental.pallas import tpu as pltpu
from jax.sharding import PartitionSpec as P

SUBSTEPS = 4
PITCH_PAD = 16
Y0 = 8
EARLY = 2
LAG = 3
MESH = pl.DeviceIdType.MESH


def kernel(
    n_x, n_y, sub_ref, up_ref, dif_hbm, dec_hbm, out_ref,
    field, uptake, faces, halos, front_sem, bulk_sem, send_sem, recv_sem,
    dif_ref, dec_ref, ready,
):
    count, cx, cy, cz = sub_ref.shape
    pitch = cy + PITCH_PAD
    out_rows = out_ref.reshape(count, cx * cy, cz)
    rows = field.reshape(SUBSTEPS, count, (cx + 2) * pitch, cz)
    gx, gy = lax.axis_index("gx"), lax.axis_index("gy")
    low_x, high_x = lax.rem(gx + n_x - 1, n_x), lax.rem(gx + 1, n_x)
    low_y, high_y = lax.rem(gy + n_y - 1, n_y), lax.rem(gy + 1, n_y)
    inner = pl.ds(Y0, cy)
    along_x = (low_x, high_x)

    shell = 2 * (cx + cy)
    flat = field.reshape(SUBSTEPS * count * (cx + 2) * pitch, cz)

    def front(s, group):
        pairs = (
            (sub_ref.at[s, :, 0, :], faces.at[0, s, 0]),
            (sub_ref.at[s, :, cy - 1, :], faces.at[0, s, 1]),
            (sub_ref.at[s, 0], field.at[0, s, 1, inner, :]),
            (sub_ref.at[s, cx - 1], field.at[0, s, cx, inner, :]),
        )
        return [pltpu.make_async_copy(src, dst, front_sem.at[group]) for src, dst in pairs]

    def bulk(s):
        return pltpu.make_async_copy(
            sub_ref.at[s, pl.ds(1, cx - 2)], field.at[0, s, pl.ds(2, cx - 2), inner, :], bulk_sem
        )

    def await_rows(n, sem):
        span = flat.at[pl.ds(0, n), :]
        pltpu.make_async_copy(span, span, sem).wait()

    def remote(t, s, src, dst, target):
        return pltpu.make_async_remote_copy(
            src_ref=src, dst_ref=dst, send_sem=send_sem,
            recv_sem=recv_sem.at[t % 2, s], device_id=target, device_id_type=MESH,
        )

    def y_sends(t, s):
        return [
            remote(t, s, faces.at[t, s, 0], halos.at[t, s, 0], (gx, low_y)),
            remote(t, s, faces.at[t, s, 1], halos.at[t, s, 1], (gx, high_y)),
        ]

    def x_send(t, s, k):
        here = field.at[t, s]
        if k == 0:
            return remote(t, s, here.at[1, inner, :], here.at[cx + 1, inner, :], (low_x, gy))
        return remote(t, s, here.at[cx, inner, :], here.at[0, inner, :], (high_x, gy))

    def make_faces(t, s):
        for i in range(cx // 8):
            top = (1 + 8 * i) * pitch + Y0
            faces[t, s, 0, pl.ds(8 * i, 8), :] = rows[t, s, pl.ds(top, 8, stride=pitch), :]
            faces[t, s, 1, pl.ds(8 * i, 8), :] = rows[
                t, s, pl.ds(top + cy - 1, 8, stride=pitch), :
            ]

    def step(t, s, ghosts, first=0, last=None):
        last = cx if last is None else last
        diffuse = dif_ref[s]
        keep = 1.0 - 6.0 * diffuse
        decay = dec_ref[s]
        zero = jnp.zeros((8, cz), jnp.float32)
        sublane = lax.broadcasted_iota(jnp.int32, (8, cz), 0)
        for y in range(0, cy, 8):
            below = field[t, s, first, pl.ds(Y0 + y, 8), :] if ghosts else zero
            center = field[t, s, first + 1, pl.ds(Y0 + y, 8), :]
            for x in range(first, last):
                if ghosts or x + 1 < cx:
                    above = field[t, s, x + 2, pl.ds(Y0 + y, 8), :]
                else:
                    above = zero
                total = below + above
                left = field[t, s, x + 1, pl.ds(Y0 + y - 1, 8), :]
                right = field[t, s, x + 1, pl.ds(Y0 + y + 1, 8), :]
                if not ghosts and y == 0:
                    left = jnp.where(sublane == 0, 0.0, left)
                if not ghosts and y + 8 == cy:
                    right = jnp.where(sublane == 7, 0.0, right)
                total = total + (left + right)
                total = total + (pltpu.roll(center, 1, 1) + pltpu.roll(center, cz - 1, 1))
                factor = keep - decay * uptake[x, pl.ds(y, 8), :]
                value = diffuse * total + factor * center
                if t + 1 < SUBSTEPS:
                    field[t + 1, s, x + 1, pl.ds(Y0 + y, 8), :] = value
                else:
                    out_ref[s, x, pl.ds(y, 8), :] = value
                below, center = center, above

    upward = jnp.logical_and(lax.rem(gy, 2) == 1, gy < n_y - 1)
    yielding = {
        (SUBSTEPS - 2, 1): (upward, LAG),
        (SUBSTEPS - 1, 1): (upward, LAG),
        (SUBSTEPS - 1, 0): (gy == n_y - 2, LAG + 1),
    }

    def send_if(condition, t, s, k):
        @pl.when(condition)
        def _():
            y_sends(t, s)[k].start()

    def send_lagging(t, s):
        for k in range(2):
            if (t, k) in yielding:
                give_way, lag = yielding[t, k]
                send_if(jnp.logical_and(give_way, s < lag), t, count - lag + s, k)

    def unit(t, s):
        send_lagging(t, s)
        await_rows(shell, recv_sem.at[t % 2, s])
        for i in range(cx // 8):
            top = (1 + 8 * i) * pitch + Y0
            rows[t, s, pl.ds(top + cy, 8, stride=pitch), :] = halos[t, s, 0, pl.ds(8 * i, 8), :]
            rows[t, s, pl.ds(top - 1, 8, stride=pitch), :] = halos[t, s, 1, pl.ds(8 * i, 8), :]
        step(t, s, True, 0, 1)
        step(t, s, True, cx - 1, cx)
        for k in range(2):
            x_send(t + 1, s, k).start()
        step(t, s, True, 1, cx - 1)
        make_faces(t + 1, s)
        for k in range(2):
            if (t + 1, k) in yielding:
                give_way, lag = yielding[t + 1, k]
                send_if(jnp.logical_not(give_way), t + 1, s, k)
                send_if(jnp.logical_and(give_way, s >= lag), t + 1, s - lag, k)
            else:
                y_sends(t + 1, s)[k].start()

    def last_unit(t, s):
        send_lagging(t, s)
        step(t, s, False)
        await_rows(shell, recv_sem.at[t % 2, s])
        diffuse = dif_ref[s]
        for x, ghost in ((0, 0), (cx - 1, cx + 1)):
            out_ref[s, x] += diffuse * field[t, s, ghost, inner, :]
        for i in range(cx // 8):
            for k, y in ((0, cy - 1), (1, 0)):
                edge = pl.ds(8 * i * cy + y, 8, stride=cy)
                out_rows[s, edge, :] += diffuse * halos[t, s, k, pl.ds(8 * i, 8), :]

    def run(first, last, body):
        def wrapped(s, carry):
            body(s)
            return carry

        lax.fori_loop(first, last, wrapped, 0)

    barrier = pltpu.get_barrier_semaphore()
    for target in ((gx, low_y), (gx, high_y)):
        pl.semaphore_signal(barrier, inc=1, device_id=target, device_id_type=MESH)
    for other in along_x:

        @pl.when(other > gx)
        def _():
            pl.semaphore_signal(barrier, inc=1, device_id=(other, gy), device_id_type=MESH)

    for first, last, group in ((0, EARLY, 0), (EARLY, count, 1)):

        def begin(s):
            for copy in front(s, group):
                copy.start()

        run(first, last, begin)
    run(0, count, lambda s: bulk(s).start())
    pltpu.make_async_copy(up_ref, uptake, bulk_sem).start()

    def launch(s):
        for copy in y_sends(0, s):
            copy.start()
        for k, other in enumerate(along_x):

            @pl.when(other < gx)
            def _():
                x_send(0, s, k).start()

    n_lower = sum((other < gx).astype(jnp.int32) for other in along_x)
    pl.semaphore_wait(barrier, 2 + n_lower)
    for k, other in enumerate(along_x):

        @pl.when(other < gx)
        def _():
            pl.semaphore_signal(
                ready.at[1 - k], inc=1, device_id=(other, gy), device_id_type=MESH
            )

    for first, last, group in ((0, EARLY, 0), (EARLY, count, 1)):
        await_rows((last - first) * shell, front_sem.at[group])
        run(first, last, launch)
    scalar_copies = [
        pltpu.make_async_copy(dif_hbm, dif_ref, front_sem.at[0]),
        pltpu.make_async_copy(dec_hbm, dec_ref, front_sem.at[1]),
    ]
    for copy in scalar_copies:
        copy.start()
    for k, other in ((1, high_x), (0, low_x)):

        @pl.when(other > gx)
        def _():
            pl.semaphore_wait(ready.at[k], 1)
            run(0, count, lambda s: x_send(0, s, k).start())

    await_rows(count * (cx - 2) * cy + cx * cy, bulk_sem)
    for copy in scalar_copies:
        copy.wait()
    for t in range(SUBSTEPS - 1):
        run(0, count, lambda s: unit(t, s))
    run(0, count, lambda s: last_unit(SUBSTEPS - 1, s))
    await_rows(SUBSTEPS * count * shell, send_sem)


def solution(mesh):
    n_x, n_y = mesh.shape["gx"], mesh.shape["gy"]

    def local(substrates, uptake, diffusion, decay_rate):
        count, cx, cy, cz = substrates.shape
        hbm_spec = pl.BlockSpec(memory_space=pltpu.HBM)
        return pl.pallas_call(
            functools.partial(kernel, n_x, n_y),
            out_shape=jax.ShapeDtypeStruct(substrates.shape, substrates.dtype),
            in_specs=[hbm_spec] * 4,
            out_specs=pl.BlockSpec(memory_space=pltpu.VMEM),
            scratch_shapes=[
                pltpu.VMEM((SUBSTEPS, count, cx + 2, cy + PITCH_PAD, cz), jnp.float32),
                pltpu.VMEM((cx, cy, cz), jnp.float32),
                pltpu.VMEM((SUBSTEPS, count, 2, cx, cz), jnp.float32),
                pltpu.VMEM((SUBSTEPS, count, 2, cx, cz), jnp.float32),
                pltpu.SemaphoreType.DMA((2,)),
                pltpu.SemaphoreType.DMA,
                pltpu.SemaphoreType.DMA,
                pltpu.SemaphoreType.DMA((2, count)),
                pltpu.SMEM((count,), jnp.float32),
                pltpu.SMEM((count,), jnp.float32),
                pltpu.SemaphoreType.REGULAR((2,)),
            ],
            compiler_params=pltpu.CompilerParams(
                collective_id=0, has_side_effects=True, vmem_limit_bytes=44 * 1024 * 1024
            ),
        )(*[pltpu.with_memory_space_constraint(v, pltpu.HBM) for v in (substrates, uptake, diffusion, decay_rate)])

    placed = (P(None, "gx", "gy", None), P("gx", "gy", None), P(), P())
    return jax.shard_map(
        local, mesh=mesh, in_specs=placed, out_specs=P(None, "gx", "gy", None), check_vma=False
    )
```

```python
import functools

import jax
import jax.numpy as jnp
from jax import lax
from jax.experimental import pallas as pl
from jax.experimental.pallas import tpu as pltpu
from jax.sharding import PartitionSpec as P

SUBSTEPS = 4
PITCH_PAD = 16
Y0 = 8
EARLY = 2
LAG = 3
MESH = pl.DeviceIdType.MESH


def kernel(
    n_x, n_y, sub_ref, up_ref, dif_hbm, dec_hbm, out_ref,
    field, uptake, faces, halos, front_sem, bulk_sem, send_sem, recv_sem,
    dif_ref, dec_ref, ready,
):
    count, cx, cy, cz = sub_ref.shape
    pitch = cy + PITCH_PAD
    out_rows = out_ref.reshape(count, cx * cy, cz)
    rows = field.reshape(SUBSTEPS, count, (cx + 2) * pitch, cz)
    gx, gy = lax.axis_index("gx"), lax.axis_index("gy")
    low_x, high_x = lax.rem(gx + n_x - 1, n_x), lax.rem(gx + 1, n_x)
    low_y, high_y = lax.rem(gy + n_y - 1, n_y), lax.rem(gy + 1, n_y)
    inner = pl.ds(Y0, cy)
    along_x = (low_x, high_x)

    shell = 2 * (cx + cy)
    flat = field.reshape(SUBSTEPS * count * (cx + 2) * pitch, cz)

    def front(s, group):
        pairs = (
            (sub_ref.at[s, :, 0, :], faces.at[0, s, 0]),
            (sub_ref.at[s, :, cy - 1, :], faces.at[0, s, 1]),
            (sub_ref.at[s, 0], field.at[0, s, 1, inner, :]),
            (sub_ref.at[s, cx - 1], field.at[0, s, cx, inner, :]),
        )
        return [pltpu.make_async_copy(src, dst, front_sem.at[group]) for src, dst in pairs]

    def bulk(s):
        return pltpu.make_async_copy(
            sub_ref.at[s, pl.ds(1, cx - 2)], field.at[0, s, pl.ds(2, cx - 2), inner, :], bulk_sem
        )

    def await_rows(n, sem):
        span = flat.at[pl.ds(0, n), :]
        pltpu.make_async_copy(span, span, sem).wait()

    def remote(t, s, src, dst, target):
        return pltpu.make_async_remote_copy(
            src_ref=src, dst_ref=dst, send_sem=send_sem,
            recv_sem=recv_sem.at[t % 2, s], device_id=target, device_id_type=MESH,
        )

    def y_sends(t, s):
        return [
            remote(t, s, faces.at[t, s, 0], halos.at[t, s, 0], (gx, low_y)),
            remote(t, s, faces.at[t, s, 1], halos.at[t, s, 1], (gx, high_y)),
        ]

    def x_send(t, s, k):
        here = field.at[t, s]
        if k == 0:
            return remote(t, s, here.at[1, inner, :], here.at[cx + 1, inner, :], (low_x, gy))
        return remote(t, s, here.at[cx, inner, :], here.at[0, inner, :], (high_x, gy))

    def make_faces(t, s):
        for i in range(cx // 8):
            top = (1 + 8 * i) * pitch + Y0
            faces[t, s, 0, pl.ds(8 * i, 8), :] = rows[t, s, pl.ds(top, 8, stride=pitch), :]
            faces[t, s, 1, pl.ds(8 * i, 8), :] = rows[
                t, s, pl.ds(top + cy - 1, 8, stride=pitch), :
            ]

    def step(t, s, ghosts, first=0, last=None):
        last = cx if last is None else last
        diffuse = dif_ref[s]
        keep = 1.0 - 6.0 * diffuse
        decay = dec_ref[s]
        zero = jnp.zeros((8, cz), jnp.float32)
        sublane = lax.broadcasted_iota(jnp.int32, (8, cz), 0)
        for y in range(0, cy, 8):
            below = field[t, s, first, pl.ds(Y0 + y, 8), :] if ghosts else zero
            center = field[t, s, first + 1, pl.ds(Y0 + y, 8), :]
            for x in range(first, last):
                if ghosts or x + 1 < cx:
                    above = field[t, s, x + 2, pl.ds(Y0 + y, 8), :]
                else:
                    above = zero
                total = below + above
                left = field[t, s, x + 1, pl.ds(Y0 + y - 1, 8), :]
                right = field[t, s, x + 1, pl.ds(Y0 + y + 1, 8), :]
                if not ghosts and y == 0:
                    left = jnp.where(sublane == 0, 0.0, left)
                if not ghosts and y + 8 == cy:
                    right = jnp.where(sublane == 7, 0.0, right)
                total = total + (left + right)
                total = total + (pltpu.roll(center, 1, 1) + pltpu.roll(center, cz - 1, 1))
                factor = keep - decay * uptake[x, pl.ds(y, 8), :]
                value = diffuse * total + factor * center
                if t + 1 < SUBSTEPS:
                    field[t + 1, s, x + 1, pl.ds(Y0 + y, 8), :] = value
                else:
                    out_ref[s, x, pl.ds(y, 8), :] = value
                below, center = center, above

    upward = jnp.logical_and(lax.rem(gy, 2) == 1, gy < n_y - 1)
    yielding = {
        (SUBSTEPS - 2, 1): (upward, LAG),
        (SUBSTEPS - 1, 1): (upward, LAG),
        (SUBSTEPS - 2, 0): (gy == n_y - 2, LAG),
        (SUBSTEPS - 1, 0): (gy == n_y - 2, LAG + 1),
    }

    def send_if(condition, t, s, k):
        @pl.when(condition)
        def _():
            y_sends(t, s)[k].start()

    def send_lagging(t, s):
        for k in range(2):
            if (t, k) in yielding:
                give_way, lag = yielding[t, k]
                send_if(jnp.logical_and(give_way, s < lag), t, count - lag + s, k)

    def unit(t, s):
        send_lagging(t, s)
        await_rows(shell, recv_sem.at[t % 2, s])
        def place(i):
            top = (1 + 8 * i) * pitch + Y0
            rows[t, s, pl.ds(top + cy, 8, stride=pitch), :] = halos[t, s, 0, pl.ds(8 * i, 8), :]
            rows[t, s, pl.ds(top - 1, 8, stride=pitch), :] = halos[t, s, 1, pl.ds(8 * i, 8), :]

        place(0)
        place(cx // 8 - 1)
        step(t, s, True, 0, 1)
        step(t, s, True, cx - 1, cx)
        for k in range(2):
            x_send(t + 1, s, k).start()
        for i in range(1, cx // 8 - 1):
            place(i)
        step(t, s, True, 1, cx - 1)
        make_faces(t + 1, s)
        for k in range(2):
            if (t + 1, k) in yielding:
                give_way, lag = yielding[t + 1, k]
                send_if(jnp.logical_not(give_way), t + 1, s, k)
                send_if(jnp.logical_and(give_way, s >= lag), t + 1, s - lag, k)
            else:
                y_sends(t + 1, s)[k].start()

    def last_unit(t, s):
        send_lagging(t, s)
        step(t, s, False)
        await_rows(shell, recv_sem.at[t % 2, s])
        diffuse = dif_ref[s]
        for x, ghost in ((0, 0), (cx - 1, cx + 1)):
            out_ref[s, x] += diffuse * field[t, s, ghost, inner, :]
        for i in range(cx // 8):
            for k, y in ((0, cy - 1), (1, 0)):
                edge = pl.ds(8 * i * cy + y, 8, stride=cy)
                out_rows[s, edge, :] += diffuse * halos[t, s, k, pl.ds(8 * i, 8), :]

    def run(first, last, body):
        def wrapped(s, carry):
            body(s)
            return carry

        lax.fori_loop(first, last, wrapped, 0)

    barrier = pltpu.get_barrier_semaphore()
    for target in ((gx, low_y), (gx, high_y)):
        pl.semaphore_signal(barrier, inc=1, device_id=target, device_id_type=MESH)
    for other in along_x:

        @pl.when(other > gx)
        def _():
            pl.semaphore_signal(barrier, inc=1, device_id=(other, gy), device_id_type=MESH)

    for first, last, group in ((0, EARLY, 0), (EARLY, count, 1)):

        def begin(s):
            for copy in front(s, group):
                copy.start()

        run(first, last, begin)
    run(0, count, lambda s: bulk(s).start())
    pltpu.make_async_copy(up_ref, uptake, bulk_sem).start()

    def launch(s):
        for copy in y_sends(0, s):
            copy.start()
        for k, other in enumerate(along_x):

            @pl.when(other < gx)
            def _():
                x_send(0, s, k).start()

    n_lower = sum((other < gx).astype(jnp.int32) for other in along_x)
    pl.semaphore_wait(barrier, 2 + n_lower)
    for k, other in enumerate(along_x):

        @pl.when(other < gx)
        def _():
            pl.semaphore_signal(
                ready.at[1 - k], inc=1, device_id=(other, gy), device_id_type=MESH
            )

    for first, last, group in ((0, EARLY, 0), (EARLY, count, 1)):
        await_rows((last - first) * shell, front_sem.at[group])
        run(first, last, launch)
    scalar_copies = [
        pltpu.make_async_copy(dif_hbm, dif_ref, front_sem.at[0]),
        pltpu.make_async_copy(dec_hbm, dec_ref, front_sem.at[1]),
    ]
    for copy in scalar_copies:
        copy.start()
    for k, other in ((1, high_x), (0, low_x)):

        @pl.when(other > gx)
        def _():
            pl.semaphore_wait(ready.at[k], 1)
            run(0, count, lambda s: x_send(0, s, k).start())

    await_rows(count * (cx - 2) * cy + cx * cy, bulk_sem)
    for copy in scalar_copies:
        copy.wait()
    for t in range(SUBSTEPS - 1):
        run(0, count, lambda s: unit(t, s))
    run(0, count, lambda s: last_unit(SUBSTEPS - 1, s))
    await_rows(SUBSTEPS * count * shell, send_sem)


def solution(mesh):
    n_x, n_y = mesh.shape["gx"], mesh.shape["gy"]

    def local(substrates, uptake, diffusion, decay_rate):
        count, cx, cy, cz = substrates.shape
        hbm_spec = pl.BlockSpec(memory_space=pltpu.HBM)
        return pl.pallas_call(
            functools.partial(kernel, n_x, n_y),
            out_shape=jax.ShapeDtypeStruct(substrates.shape, substrates.dtype),
            in_specs=[hbm_spec] * 4,
            out_specs=pl.BlockSpec(memory_space=pltpu.VMEM),
            scratch_shapes=[
                pltpu.VMEM((SUBSTEPS, count, cx + 2, cy + PITCH_PAD, cz), jnp.float32),
                pltpu.VMEM((cx, cy, cz), jnp.float32),
                pltpu.VMEM((SUBSTEPS, count, 2, cx, cz), jnp.float32),
                pltpu.VMEM((SUBSTEPS, count, 2, cx, cz), jnp.float32),
                pltpu.SemaphoreType.DMA((2,)),
                pltpu.SemaphoreType.DMA,
                pltpu.SemaphoreType.DMA,
                pltpu.SemaphoreType.DMA((2, count)),
                pltpu.SMEM((count,), jnp.float32),
                pltpu.SMEM((count,), jnp.float32),
                pltpu.SemaphoreType.REGULAR((2,)),
            ],
            compiler_params=pltpu.CompilerParams(
                collective_id=0, has_side_effects=True, vmem_limit_bytes=44 * 1024 * 1024
            ),
        )(*[pltpu.with_memory_space_constraint(v, pltpu.HBM) for v in (substrates, uptake, diffusion, decay_rate)])

    placed = (P(None, "gx", "gy", None), P("gx", "gy", None), P(), P())
    return jax.shard_map(
        local, mesh=mesh, in_specs=placed, out_specs=P(None, "gx", "gy", None), check_vma=False
    )
```

```python
import functools

import jax
import jax.numpy as jnp
from jax import lax
from jax.experimental import pallas as pl
from jax.experimental.pallas import tpu as pltpu
from jax.sharding import PartitionSpec as P

SUBSTEPS = 4
PITCH_PAD = 16
Y0 = 8
EARLY = 2
LAG = 3
MESH = pl.DeviceIdType.MESH


def kernel(
    n_x, n_y, sub_ref, up_ref, dif_hbm, dec_hbm, out_ref,
    field, uptake, faces, halos, front_sem, bulk_sem, send_sem, recv_sem,
    dif_ref, dec_ref, ready,
):
    count, cx, cy, cz = sub_ref.shape
    pitch = cy + PITCH_PAD
    out_rows = out_ref.reshape(count, cx * cy, cz)
    rows = field.reshape(SUBSTEPS, count, (cx + 2) * pitch, cz)
    gx, gy = lax.axis_index("gx"), lax.axis_index("gy")
    low_x, high_x = lax.rem(gx + n_x - 1, n_x), lax.rem(gx + 1, n_x)
    low_y, high_y = lax.rem(gy + n_y - 1, n_y), lax.rem(gy + 1, n_y)
    inner = pl.ds(Y0, cy)
    along_x = (low_x, high_x)

    shell = 2 * (cx + cy)
    flat = field.reshape(SUBSTEPS * count * (cx + 2) * pitch, cz)

    def front(s, group):
        pairs = (
            (sub_ref.at[s, :, 0, :], faces.at[0, s, 0]),
            (sub_ref.at[s, :, cy - 1, :], faces.at[0, s, 1]),
            (sub_ref.at[s, 0], field.at[0, s, 1, inner, :]),
            (sub_ref.at[s, cx - 1], field.at[0, s, cx, inner, :]),
        )
        return [pltpu.make_async_copy(src, dst, front_sem.at[group]) for src, dst in pairs]

    def bulk(s):
        return pltpu.make_async_copy(
            sub_ref.at[s, pl.ds(1, cx - 2)], field.at[0, s, pl.ds(2, cx - 2), inner, :], bulk_sem
        )

    def await_rows(n, sem):
        span = flat.at[pl.ds(0, n), :]
        pltpu.make_async_copy(span, span, sem).wait()

    def remote(t, s, src, dst, target):
        return pltpu.make_async_remote_copy(
            src_ref=src, dst_ref=dst, send_sem=send_sem,
            recv_sem=recv_sem.at[t % 2, s], device_id=target, device_id_type=MESH,
        )

    def y_sends(t, s):
        return [
            remote(t, s, faces.at[t, s, 0], halos.at[t, s, 0], (gx, low_y)),
            remote(t, s, faces.at[t, s, 1], halos.at[t, s, 1], (gx, high_y)),
        ]

    def x_send(t, s, k):
        here = field.at[t, s]
        if k == 0:
            return remote(t, s, here.at[1, inner, :], here.at[cx + 1, inner, :], (low_x, gy))
        return remote(t, s, here.at[cx, inner, :], here.at[0, inner, :], (high_x, gy))

    def make_faces(t, s):
        for i in range(cx // 8):
            top = (1 + 8 * i) * pitch + Y0
            faces[t, s, 0, pl.ds(8 * i, 8), :] = rows[t, s, pl.ds(top, 8, stride=pitch), :]
            faces[t, s, 1, pl.ds(8 * i, 8), :] = rows[
                t, s, pl.ds(top + cy - 1, 8, stride=pitch), :
            ]

    def step(t, s, ghosts, first=0, last=None):
        last = cx if last is None else last
        diffuse = dif_ref[s]
        keep = 1.0 - 6.0 * diffuse
        decay = dec_ref[s]
        zero = jnp.zeros((8, cz), jnp.float32)
        sublane = lax.broadcasted_iota(jnp.int32, (8, cz), 0)
        for y in range(0, cy, 8):
            below = field[t, s, first, pl.ds(Y0 + y, 8), :] if ghosts else zero
            center = field[t, s, first + 1, pl.ds(Y0 + y, 8), :]
            for x in range(first, last):
                if ghosts or x + 1 < cx:
                    above = field[t, s, x + 2, pl.ds(Y0 + y, 8), :]
                else:
                    above = zero
                total = below + above
                left = field[t, s, x + 1, pl.ds(Y0 + y - 1, 8), :]
                right = field[t, s, x + 1, pl.ds(Y0 + y + 1, 8), :]
                if not ghosts and y == 0:
                    left = jnp.where(sublane == 0, 0.0, left)
                if not ghosts and y + 8 == cy:
                    right = jnp.where(sublane == 7, 0.0, right)
                total = total + (left + right)
                total = total + (pltpu.roll(center, 1, 1) + pltpu.roll(center, cz - 1, 1))
                factor = keep - decay * uptake[x, pl.ds(y, 8), :]
                value = diffuse * total + factor * center
                if t + 1 < SUBSTEPS:
                    field[t + 1, s, x + 1, pl.ds(Y0 + y, 8), :] = value
                else:
                    out_ref[s, x, pl.ds(y, 8), :] = value
                below, center = center, above

    upward = jnp.logical_and(lax.rem(gy, 2) == 1, gy < n_y - 1)
    yielding = {
        (SUBSTEPS - 2, 1): (upward, LAG),
        (SUBSTEPS - 1, 1): (upward, LAG),
        (SUBSTEPS - 2, 0): (gy == n_y - 2, LAG),
        (SUBSTEPS - 1, 0): (gy == n_y - 2, LAG + 1),
    }

    def send_if(condition, t, s, k):
        @pl.when(condition)
        def _():
            y_sends(t, s)[k].start()

    def send_lagging(t, s):
        for k in range(2):
            if (t, k) in yielding:
                give_way, lag = yielding[t, k]
                send_if(jnp.logical_and(give_way, s < lag), t, count - lag + s, k)

    def unit(t, s):
        send_lagging(t, s)
        await_rows(shell, recv_sem.at[t % 2, s])
        def place(i):
            top = (1 + 8 * i) * pitch + Y0
            rows[t, s, pl.ds(top + cy, 8, stride=pitch), :] = halos[t, s, 0, pl.ds(8 * i, 8), :]
            rows[t, s, pl.ds(top - 1, 8, stride=pitch), :] = halos[t, s, 1, pl.ds(8 * i, 8), :]

        place(0)
        place(cx // 8 - 1)
        step(t, s, True, 0, 1)
        step(t, s, True, cx - 1, cx)
        for k in (1, 0):
            x_send(t + 1, s, k).start()
        for i in range(1, cx // 8 - 1):
            place(i)
        step(t, s, True, 1, cx - 1)
        make_faces(t + 1, s)
        for k in range(2):
            if (t + 1, k) in yielding:
                give_way, lag = yielding[t + 1, k]
                send_if(jnp.logical_not(give_way), t + 1, s, k)
                send_if(jnp.logical_and(give_way, s >= lag), t + 1, s - lag, k)
            else:
                y_sends(t + 1, s)[k].start()

    def last_unit(t, s):
        send_lagging(t, s)
        step(t, s, False)
        await_rows(shell, recv_sem.at[t % 2, s])
        diffuse = dif_ref[s]
        for x, ghost in ((0, 0), (cx - 1, cx + 1)):
            out_ref[s, x] += diffuse * field[t, s, ghost, inner, :]
        for i in range(cx // 8):
            for k, y in ((0, cy - 1), (1, 0)):
                edge = pl.ds(8 * i * cy + y, 8, stride=cy)
                out_rows[s, edge, :] += diffuse * halos[t, s, k, pl.ds(8 * i, 8), :]

    def run(first, last, body):
        def wrapped(s, carry):
            body(s)
            return carry

        lax.fori_loop(first, last, wrapped, 0)

    barrier = pltpu.get_barrier_semaphore()
    for target in ((gx, low_y), (gx, high_y)):
        pl.semaphore_signal(barrier, inc=1, device_id=target, device_id_type=MESH)
    for other in along_x:

        @pl.when(other > gx)
        def _():
            pl.semaphore_signal(barrier, inc=1, device_id=(other, gy), device_id_type=MESH)

    for first, last, group in ((0, EARLY, 0), (EARLY, count, 1)):

        def begin(s):
            for copy in front(s, group):
                copy.start()

        run(first, last, begin)
    run(0, count, lambda s: bulk(s).start())
    pltpu.make_async_copy(up_ref, uptake, bulk_sem).start()

    def launch(s):
        for copy in y_sends(0, s):
            copy.start()
        for k, other in enumerate(along_x):

            @pl.when(other < gx)
            def _():
                x_send(0, s, k).start()

    n_lower = sum((other < gx).astype(jnp.int32) for other in along_x)
    pl.semaphore_wait(barrier, 2 + n_lower)
    for k, other in enumerate(along_x):

        @pl.when(other < gx)
        def _():
            pl.semaphore_signal(
                ready.at[1 - k], inc=1, device_id=(other, gy), device_id_type=MESH
            )

    for first, last, group in ((0, EARLY, 0), (EARLY, count, 1)):
        await_rows((last - first) * shell, front_sem.at[group])
        run(first, last, launch)
    scalar_copies = [
        pltpu.make_async_copy(dif_hbm, dif_ref, front_sem.at[0]),
        pltpu.make_async_copy(dec_hbm, dec_ref, front_sem.at[1]),
    ]
    for copy in scalar_copies:
        copy.start()
    for k, other in ((1, high_x), (0, low_x)):

        @pl.when(other > gx)
        def _():
            pl.semaphore_wait(ready.at[k], 1)
            run(0, count, lambda s: x_send(0, s, k).start())

    await_rows(count * (cx - 2) * cy + cx * cy, bulk_sem)
    for copy in scalar_copies:
        copy.wait()
    for t in range(SUBSTEPS - 1):
        run(0, count, lambda s: unit(t, s))
    run(0, count, lambda s: last_unit(SUBSTEPS - 1, s))
    await_rows(SUBSTEPS * count * shell, send_sem)


def solution(mesh):
    n_x, n_y = mesh.shape["gx"], mesh.shape["gy"]

    def local(substrates, uptake, diffusion, decay_rate):
        count, cx, cy, cz = substrates.shape
        hbm_spec = pl.BlockSpec(memory_space=pltpu.HBM)
        return pl.pallas_call(
            functools.partial(kernel, n_x, n_y),
            out_shape=jax.ShapeDtypeStruct(substrates.shape, substrates.dtype),
            in_specs=[hbm_spec] * 4,
            out_specs=pl.BlockSpec(memory_space=pltpu.VMEM),
            scratch_shapes=[
                pltpu.VMEM((SUBSTEPS, count, cx + 2, cy + PITCH_PAD, cz), jnp.float32),
                pltpu.VMEM((cx, cy, cz), jnp.float32),
                pltpu.VMEM((SUBSTEPS, count, 2, cx, cz), jnp.float32),
                pltpu.VMEM((SUBSTEPS, count, 2, cx, cz), jnp.float32),
                pltpu.SemaphoreType.DMA((2,)),
                pltpu.SemaphoreType.DMA,
                pltpu.SemaphoreType.DMA,
                pltpu.SemaphoreType.DMA((2, count)),
                pltpu.SMEM((count,), jnp.float32),
                pltpu.SMEM((count,), jnp.float32),
                pltpu.SemaphoreType.REGULAR((2,)),
            ],
            compiler_params=pltpu.CompilerParams(
                collective_id=0, has_side_effects=True, vmem_limit_bytes=44 * 1024 * 1024
            ),
        )(*[pltpu.with_memory_space_constraint(v, pltpu.HBM) for v in (substrates, uptake, diffusion, decay_rate)])

    placed = (P(None, "gx", "gy", None), P("gx", "gy", None), P(), P())
    return jax.shard_map(
        local, mesh=mesh, in_specs=placed, out_specs=P(None, "gx", "gy", None), check_vma=False
    )
```

```python
import functools

import jax
import jax.numpy as jnp
from jax import lax
from jax.experimental import pallas as pl
from jax.experimental.pallas import tpu as pltpu
from jax.sharding import PartitionSpec as P

SUBSTEPS = 4
PITCH_PAD = 16
Y0 = 8
EARLY = 2
LAG = 3
MESH = pl.DeviceIdType.MESH


def kernel(
    n_x, n_y, sub_ref, up_ref, dif_hbm, dec_hbm, out_ref,
    field, uptake, faces, halos, front_sem, bulk_sem, send_sem, recv_sem,
    dif_ref, dec_ref, ready,
):
    count, cx, cy, cz = sub_ref.shape
    pitch = cy + PITCH_PAD
    out_rows = out_ref.reshape(count, cx * cy, cz)
    rows = field.reshape(SUBSTEPS, count, (cx + 2) * pitch, cz)
    gx, gy = lax.axis_index("gx"), lax.axis_index("gy")
    low_x, high_x = lax.rem(gx + n_x - 1, n_x), lax.rem(gx + 1, n_x)
    low_y, high_y = lax.rem(gy + n_y - 1, n_y), lax.rem(gy + 1, n_y)
    inner = pl.ds(Y0, cy)
    along_x = (low_x, high_x)

    shell = 2 * (cx + cy)
    flat = field.reshape(SUBSTEPS * count * (cx + 2) * pitch, cz)

    def front(s, group):
        pairs = (
            (sub_ref.at[s, :, 0, :], faces.at[0, s, 0]),
            (sub_ref.at[s, :, cy - 1, :], faces.at[0, s, 1]),
            (sub_ref.at[s, 0], field.at[0, s, 1, inner, :]),
            (sub_ref.at[s, cx - 1], field.at[0, s, cx, inner, :]),
        )
        return [pltpu.make_async_copy(src, dst, front_sem.at[group]) for src, dst in pairs]

    def bulk(s):
        return pltpu.make_async_copy(
            sub_ref.at[s, pl.ds(1, cx - 2)], field.at[0, s, pl.ds(2, cx - 2), inner, :], bulk_sem
        )

    def await_rows(n, sem):
        span = flat.at[pl.ds(0, n), :]
        pltpu.make_async_copy(span, span, sem).wait()

    def remote(t, s, src, dst, target):
        return pltpu.make_async_remote_copy(
            src_ref=src, dst_ref=dst, send_sem=send_sem,
            recv_sem=recv_sem.at[t % 2, s], device_id=target, device_id_type=MESH,
        )

    def y_sends(t, s):
        return [
            remote(t, s, faces.at[t, s, 0], halos.at[t, s, 0], (gx, low_y)),
            remote(t, s, faces.at[t, s, 1], halos.at[t, s, 1], (gx, high_y)),
        ]

    def x_send(t, s, k):
        here = field.at[t, s]
        if k == 0:
            return remote(t, s, here.at[1, inner, :], here.at[cx + 1, inner, :], (low_x, gy))
        return remote(t, s, here.at[cx, inner, :], here.at[0, inner, :], (high_x, gy))

    def make_faces(t, s):
        for i in range(cx // 8):
            top = (1 + 8 * i) * pitch + Y0
            faces[t, s, 0, pl.ds(8 * i, 8), :] = rows[t, s, pl.ds(top, 8, stride=pitch), :]
            faces[t, s, 1, pl.ds(8 * i, 8), :] = rows[
                t, s, pl.ds(top + cy - 1, 8, stride=pitch), :
            ]

    def step(t, s, ghosts, first=0, last=None):
        last = cx if last is None else last
        diffuse = dif_ref[s]
        keep = 1.0 - 6.0 * diffuse
        decay = dec_ref[s]
        zero = jnp.zeros((8, cz), jnp.float32)
        sublane = lax.broadcasted_iota(jnp.int32, (8, cz), 0)
        for y in range(0, cy, 8):
            below = field[t, s, first, pl.ds(Y0 + y, 8), :] if ghosts else zero
            center = field[t, s, first + 1, pl.ds(Y0 + y, 8), :]
            for x in range(first, last):
                if ghosts or x + 1 < cx:
                    above = field[t, s, x + 2, pl.ds(Y0 + y, 8), :]
                else:
                    above = zero
                total = below + above
                left = field[t, s, x + 1, pl.ds(Y0 + y - 1, 8), :]
                right = field[t, s, x + 1, pl.ds(Y0 + y + 1, 8), :]
                if not ghosts and y == 0:
                    left = jnp.where(sublane == 0, 0.0, left)
                if not ghosts and y + 8 == cy:
                    right = jnp.where(sublane == 7, 0.0, right)
                total = total + (left + right)
                total = total + (pltpu.roll(center, 1, 1) + pltpu.roll(center, cz - 1, 1))
                factor = keep - decay * uptake[x, pl.ds(y, 8), :]
                value = diffuse * total + factor * center
                if t + 1 < SUBSTEPS:
                    field[t + 1, s, x + 1, pl.ds(Y0 + y, 8), :] = value
                else:
                    out_ref[s, x, pl.ds(y, 8), :] = value
                below, center = center, above

    upward = jnp.logical_and(lax.rem(gy, 2) == 1, gy < n_y - 1)
    yielding = {
        (SUBSTEPS - 2, 1): (upward, LAG),
        (SUBSTEPS - 1, 1): (upward, LAG),
        (SUBSTEPS - 2, 0): (gy == n_y - 2, LAG - 1),
        (SUBSTEPS - 1, 0): (gy == n_y - 2, LAG + 1),
    }

    def send_if(condition, t, s, k):
        @pl.when(condition)
        def _():
            y_sends(t, s)[k].start()

    def send_lagging(t, s):
        for k in range(2):
            if (t, k) in yielding:
                give_way, lag = yielding[t, k]
                send_if(jnp.logical_and(give_way, s < lag), t, count - lag + s, k)

    def unit(t, s):
        send_lagging(t, s)
        await_rows(shell, recv_sem.at[t % 2, s])
        def place(i):
            top = (1 + 8 * i) * pitch + Y0
            rows[t, s, pl.ds(top + cy, 8, stride=pitch), :] = halos[t, s, 0, pl.ds(8 * i, 8), :]
            rows[t, s, pl.ds(top - 1, 8, stride=pitch), :] = halos[t, s, 1, pl.ds(8 * i, 8), :]

        place(0)
        place(cx // 8 - 1)
        step(t, s, True, 0, 1)
        step(t, s, True, cx - 1, cx)
        for k in (1, 0):
            x_send(t + 1, s, k).start()
        for i in range(1, cx // 8 - 1):
            place(i)
        step(t, s, True, 1, cx - 1)
        make_faces(t + 1, s)
        for k in range(2):
            if (t + 1, k) in yielding:
                give_way, lag = yielding[t + 1, k]
                send_if(jnp.logical_not(give_way), t + 1, s, k)
                send_if(jnp.logical_and(give_way, s >= lag), t + 1, s - lag, k)
            else:
                y_sends(t + 1, s)[k].start()

    def last_unit(t, s):
        send_lagging(t, s)
        step(t, s, False)
        await_rows(shell, recv_sem.at[t % 2, s])
        diffuse = dif_ref[s]
        for x, ghost in ((0, 0), (cx - 1, cx + 1)):
            out_ref[s, x] += diffuse * field[t, s, ghost, inner, :]
        for i in range(cx // 8):
            for k, y in ((0, cy - 1), (1, 0)):
                edge = pl.ds(8 * i * cy + y, 8, stride=cy)
                out_rows[s, edge, :] += diffuse * halos[t, s, k, pl.ds(8 * i, 8), :]

    def run(first, last, body):
        def wrapped(s, carry):
            body(s)
            return carry

        lax.fori_loop(first, last, wrapped, 0)

    barrier = pltpu.get_barrier_semaphore()
    for target in ((gx, low_y), (gx, high_y)):
        pl.semaphore_signal(barrier, inc=1, device_id=target, device_id_type=MESH)
    for other in along_x:

        @pl.when(other > gx)
        def _():
            pl.semaphore_signal(barrier, inc=1, device_id=(other, gy), device_id_type=MESH)

    for first, last, group in ((0, EARLY, 0), (EARLY, count, 1)):

        def begin(s):
            for copy in front(s, group):
                copy.start()

        run(first, last, begin)
    run(0, count, lambda s: bulk(s).start())
    pltpu.make_async_copy(up_ref, uptake, bulk_sem).start()

    def launch(s):
        for copy in y_sends(0, s):
            copy.start()
        for k, other in enumerate(along_x):

            @pl.when(other < gx)
            def _():
                x_send(0, s, k).start()

    n_lower = sum((other < gx).astype(jnp.int32) for other in along_x)
    pl.semaphore_wait(barrier, 2 + n_lower)
    for k, other in enumerate(along_x):

        @pl.when(other < gx)
        def _():
            pl.semaphore_signal(
                ready.at[1 - k], inc=1, device_id=(other, gy), device_id_type=MESH
            )

    for first, last, group in ((0, EARLY, 0), (EARLY, count, 1)):
        await_rows((last - first) * shell, front_sem.at[group])
        run(first, last, launch)
    scalar_copies = [
        pltpu.make_async_copy(dif_hbm, dif_ref, front_sem.at[0]),
        pltpu.make_async_copy(dec_hbm, dec_ref, front_sem.at[1]),
    ]
    for copy in scalar_copies:
        copy.start()
    for k, other in ((1, high_x), (0, low_x)):

        @pl.when(other > gx)
        def _():
            pl.semaphore_wait(ready.at[k], 1)
            run(0, count, lambda s: x_send(0, s, k).start())

    await_rows(count * (cx - 2) * cy + cx * cy, bulk_sem)
    for copy in scalar_copies:
        copy.wait()
    for t in range(SUBSTEPS - 1):
        run(0, count, lambda s: unit(t, s))
    run(0, count, lambda s: last_unit(SUBSTEPS - 1, s))
    await_rows(SUBSTEPS * count * shell, send_sem)


def solution(mesh):
    n_x, n_y = mesh.shape["gx"], mesh.shape["gy"]

    def local(substrates, uptake, diffusion, decay_rate):
        count, cx, cy, cz = substrates.shape
        hbm_spec = pl.BlockSpec(memory_space=pltpu.HBM)
        return pl.pallas_call(
            functools.partial(kernel, n_x, n_y),
            out_shape=jax.ShapeDtypeStruct(substrates.shape, substrates.dtype),
            in_specs=[hbm_spec] * 4,
            out_specs=pl.BlockSpec(memory_space=pltpu.VMEM),
            scratch_shapes=[
                pltpu.VMEM((SUBSTEPS, count, cx + 2, cy + PITCH_PAD, cz), jnp.float32),
                pltpu.VMEM((cx, cy, cz), jnp.float32),
                pltpu.VMEM((SUBSTEPS, count, 2, cx, cz), jnp.float32),
                pltpu.VMEM((SUBSTEPS, count, 2, cx, cz), jnp.float32),
                pltpu.SemaphoreType.DMA((2,)),
                pltpu.SemaphoreType.DMA,
                pltpu.SemaphoreType.DMA,
                pltpu.SemaphoreType.DMA((2, count)),
                pltpu.SMEM((count,), jnp.float32),
                pltpu.SMEM((count,), jnp.float32),
                pltpu.SemaphoreType.REGULAR((2,)),
            ],
            compiler_params=pltpu.CompilerParams(
                collective_id=0, has_side_effects=True, vmem_limit_bytes=44 * 1024 * 1024
            ),
        )(*[pltpu.with_memory_space_constraint(v, pltpu.HBM) for v in (substrates, uptake, diffusion, decay_rate)])

    placed = (P(None, "gx", "gy", None), P("gx", "gy", None), P(), P())
    return jax.shard_map(
        local, mesh=mesh, in_specs=placed, out_specs=P(None, "gx", "gy", None), check_vma=False
    )
```
